32 devices in a mesh: lat: 8 (over y, x, core), lon: 4 (over z).
Axes of the slice: x: 2, y: 2, z: 4, core: 2. Of those that a mesh axis runs over, the one named last changes fastest.
Arguments:
- tokens: bfloat16 [4, 64, 128, 1024], P(None, 'lat', 'lon'), may hold values from -6 to 6
- qkv_weight: bfloat16 [3072, 1024], P(('lat', 'lon')), may hold values from -0.1875 to 0.1875
- proj_weight: bfloat16 [1024, 1024], P(('lat', 'lon')), may hold values from -0.1875 to 0.1875
- up_weight: bfloat16 [4096, 1024], P(('lat', 'lon')), may hold values from -0.1875 to 0.1875
- down_weight: bfloat16 [4096, 1024], P(('lat', 'lon')), may hold values from -0.09375 to 0.09375
- bias_table: float32 [225, 16], replicated, may hold values from -3 to 220, as said below
- sea_mask: int32 [64, 128], replicated, may hold values 0 or 1
Outputs:
- block_out: bfloat16 [4, 64, 128, 1024], P(None, 'lat', 'lon')
The draws below stay inside these ranges and needn't reach their ends.
Inputs may be any that keep to these rules, and one draw needn't show every extreme that they name: `bias_table`: entry [o, h] is the bias of head h for the in-window offset numbered o as in the reference program.
All inputs are finite; a program needn't handle non-finite values.
Results may differ from the reference program's by a relative error of at most 0.012.
Values may be sent and summed in bfloat16 or wider, within the bound.
A program may use at most 128 MiB of HBM per device.

```python
import jax
import jax.numpy as jnp
from jax import lax

D = 1024
HEADS = 16
MLP = 4096
BATCH = 4
RELPOS = 225
HEAD_DIM = 64
NLAT = 64
NLON = 128


def draw_bias_table(key, part):
    base_key, head_key = jax.random.split(jax.random.fold_in(key, 7))
    bias_rows = jnp.clip(jax.random.normal(base_key, (RELPOS, HEADS), jnp.float32), -3.0, 3.0)
    return bias_rows


def plant(values, stream_key, smallest, top_value):
    place = [jax.random.randint(jax.random.fold_in(stream_key, axis), (), 0, length) for axis, length in enumerate(values.shape)]
    main_axis = values.shape.index(max(values.shape))
    next_to = place[:main_axis] + [(place[main_axis] + 1) % values.shape[main_axis]] + place[main_axis + 1:]
    return values.at[tuple(place)].set(smallest).at[tuple(next_to)].set(top_value)


def shard_levels(rng, shape, pieces, least, top_value):
    level = 1.0
    for position, blocks in pieces:
        steps = jax.random.uniform(jax.random.fold_in(jax.random.fold_in(rng, 6), position), (blocks,), jnp.float32, least / len(pieces), top_value / len(pieces))
        level = level * jnp.repeat(jnp.exp(steps), shape[position] // blocks).reshape((-1,) + (1,) * (len(shape) - 1 - position))
    return level


def noise(rng, dims, deviation, reach, pieces=(), kind=jnp.bfloat16):
    drawn = jax.random.normal(rng, dims, jnp.float32) * deviation
    if len(pieces) > 0:
        drawn = shard_levels(rng, dims, pieces, -0.22, 0.18) * drawn
    return jnp.clip(drawn, min=-reach, max=reach).astype(kind)


def setup_inputs(seed: int = 0) -> dict:
    splits = jax.random.split(jax.random.key(seed), 8)
    return {
        "tokens": noise(splits[0], (BATCH, NLAT, NLON, D), 1.0, 6.0, ((1, 8), (2, 4))),
        "qkv_weight": noise(splits[1], (3 * D, D), D ** -0.5, 0.1875, ((0, 32),)),
        "proj_weight": noise(splits[2], (D, D), D ** -0.5, 0.1875, ((0, 32),)),
        "up_weight": noise(splits[3], (MLP, D), D ** -0.5, 0.1875, ((0, 32),)),
        "down_weight": noise(splits[4], (MLP, D), MLP ** -0.5, 0.09375, ((0, 32),)),
        "bias_table": draw_bias_table(jax.random.fold_in(splits[7], 71), 0),
        "sea_mask": plant((jax.random.randint(splits[6], (NLAT, NLON), 0, 4) < 3).astype(jnp.int32), jax.random.fold_in(splits[6], 1), 0, 1),
    }


def layer_norm(values):
    widened = values.astype(jnp.float32)
    centre = lax.optimization_barrier(jnp.mean(widened, axis=-1, keepdims=True))
    spread = lax.optimization_barrier(jnp.mean(jnp.square(widened - centre), axis=-1, keepdims=True))
    return ((widened - centre) * lax.rsqrt(spread + 1e-05)).astype(jnp.bfloat16)

def offsets_table():
    cell_ids = jnp.arange(64, dtype=jnp.int32)
    row_of = cell_ids // 8
    col_of = cell_ids % 8
    return (row_of[:, None] - row_of[None, :] + 7) * 15 + (col_of[:, None] - col_of[None, :] + 7)

def row_region(row_ids, total_rows):
    return jnp.where(row_ids < 4, 2, jnp.where(row_ids >= total_rows - 4, 1, 0)).astype(jnp.int32)

def reference(tokens, qkv_weight, proj_weight, up_weight, down_weight, bias_table, sea_mask):
    normed = layer_norm(tokens)
    rolled = jnp.roll(normed, (-4, -4), axis=(1, 2))
    sea_rolled = jnp.roll(sea_mask, (-4, -4), axis=(0, 1))
    pos_bias = jnp.transpose(bias_table[offsets_table()], (2, 0, 1))
    same_cell = jnp.eye(64, dtype=bool)
    windows_across = NLON // 8
    row_blocks = jnp.transpose(rolled.reshape(BATCH, NLAT // 8, 8, NLON, D), (1, 0, 2, 3, 4))
    sea_blocks = sea_rolled.reshape(NLAT // 8, 8, NLON)
    score_scale = HEAD_DIM ** (-0.5)

    def window_row(inputs):
        row_block, sea_rows, block_index = inputs
        projected = jnp.dot(row_block.reshape(-1, D), qkv_weight.T, preferred_element_type=jnp.float32).astype(jnp.bfloat16)
        windows = projected.reshape(BATCH, 8, windows_across, 8, 3 * D).transpose(0, 2, 1, 3, 4)
        windows = windows.reshape(BATCH, windows_across, 64, 3, HEADS, HEAD_DIM).astype(jnp.float32)
        queries = windows[:, :, :, 0]
        keys_here = windows[:, :, :, 1]
        values_here = windows[:, :, :, 2]
        scores = jnp.einsum('bsqhd,bskhd->bshqk', queries, keys_here) * score_scale + pos_bias[None, None]
        grid_rows = (block_index * 8 + 4 + jnp.arange(8, dtype=jnp.int32)) % NLAT
        region = jnp.repeat(row_region(grid_rows, NLAT), 8)
        sea_keep = sea_rows.reshape(8, windows_across, 8).transpose(1, 0, 2).reshape(windows_across, 64) == 1
        allowed = (region[:, None] == region[None, :])[None] & (sea_keep[:, None, :] | same_cell[None])
        scores = jnp.where(allowed[None, :, None], scores, -1e+30)
        row_top = lax.optimization_barrier(jnp.max(scores, axis=-1, keepdims=True))
        weights = jnp.exp(scores - row_top)
        attn_probs = (weights / lax.optimization_barrier(jnp.sum(weights, axis=-1, keepdims=True))).astype(jnp.bfloat16)
        context = jnp.einsum('bshqk,bskhd->bsqhd', attn_probs.astype(jnp.float32), values_here).astype(jnp.bfloat16)
        context = context.reshape(BATCH, windows_across, 8, 8, D).transpose(0, 2, 1, 3, 4)
        return context.reshape(BATCH, 8, NLON, D)
    contexts = lax.map(window_row, (row_blocks, sea_blocks, jnp.arange(NLAT // 8, dtype=jnp.int32)))
    context_grid = jnp.transpose(contexts, (1, 0, 2, 3, 4)).reshape(BATCH, NLAT, NLON, D)
    context_grid = jnp.roll(context_grid, (4, 4), axis=(1, 2))

    def finish(inputs):
        token_block, context_block = inputs
        attention_out = jnp.dot(context_block.reshape(-1, D), proj_weight.T, preferred_element_type=jnp.float32)
        attended = (token_block.reshape(-1, D).astype(jnp.float32) + attention_out).astype(jnp.bfloat16)
        normed_two = layer_norm(attended)
        hidden = jax.nn.gelu(jnp.dot(normed_two, up_weight.T, preferred_element_type=jnp.float32)).astype(jnp.bfloat16)
        result = attended.astype(jnp.float32) + jnp.dot(hidden, down_weight, preferred_element_type=jnp.float32)
        return result.astype(jnp.bfloat16).reshape(token_block.shape)
    token_rows = jnp.transpose(tokens.reshape(BATCH, NLAT // 8, 8, NLON, D), (1, 0, 2, 3, 4))
    context_rows = jnp.transpose(context_grid.reshape(BATCH, NLAT // 8, 8, NLON, D), (1, 0, 2, 3, 4))
    finished = lax.map(finish, (token_rows, context_rows))
    return jnp.transpose(finished, (1, 0, 2, 3, 4)).reshape(BATCH, NLAT, NLON, D)
```

```python
import jax
import jax.numpy as jnp
from jax import lax
from jax.experimental import pallas as pl
from jax.experimental.pallas import tpu as pltpu
from jax.sharding import PartitionSpec as P


MESH_ID = pl.DeviceIdType.MESH


def piece_rows(rows, flip):
    unit = 16 if rows % 16 == 0 else 8
    units = rows // unit
    last = (units * 3 + 6) // 13
    first = (units - last + 1) // 2
    second = units - last - first
    if flip:
        first, second = second, first
    bounds = [0, first * unit, (first + second) * unit, rows]
    return [(bounds[i], bounds[i + 1] - bounds[i]) for i in range(3)]


def split_lat(lat_size):
    inner = lat_size // 4
    return (2, inner) if lat_size % 4 == 0 else (1, lat_size // 2)


class Gather:
    def __init__(self, sizes, ins, outs, stage, send_sem, recv_sem, load_sem, order):
        self.sizes = sizes
        self.ins, self.outs, self.stage = ins, outs, stage
        self.send_sem, self.recv_sem, self.load_sem = send_sem, recv_sem, load_sem
        lat, lon = lax.axis_index("lat"), lax.axis_index("lon")
        self.core = lax.rem(lat, 2)
        chip = lax.div(lat, 2)
        self.at = {"y": lax.div(chip, sizes["x"]), "x": lax.rem(chip, sizes["x"]), "z": lon}
        self.next_sem = 0
        self.sends = []
        self.flows = []
        for turn, (index, offset) in enumerate(order):
            pieces = piece_rows(ins[index].shape[0], turn % 2 == 1)
            for axes, (start, length) in zip(("zyx", "zxy", None), pieces):
                if length == 0:
                    continue
                if axes is None:
                    axes = "xyz" if turn % 2 == 0 else "yxz"
                self.flows.append((offset, self.steps(index, axes, start, length)))
        self.length = max(offset + len(steps) for offset, steps in self.flows)

    def device(self, axis=None, move=0):
        place = dict(self.at)
        core = self.core
        if axis == "core":
            core = 1 - core
        elif axis is not None:
            place[axis] = place[axis] + move
        return ((place["y"] * self.sizes["x"] + place["x"]) * 2 + core, place["z"])

    def barrier(self):
        sem = pltpu.get_barrier_semaphore()
        count = 0
        for axis in "yxz":
            size = self.sizes[axis]
            if size == 1:
                continue
            for move in (1, size - 1):
                place = dict(self.at)
                place[axis] = lax.rem(place[axis] + move, size)
                where = (
                    (place["y"] * self.sizes["x"] + place["x"]) * 2 + self.core,
                    place["z"],
                )
                pl.semaphore_signal(sem, inc=1, device_id=where, device_id_type=MESH_ID)
                count += 1
        pl.semaphore_signal(
            sem, inc=1, device_id=self.device("core"), device_id_type=MESH_ID
        )
        pl.semaphore_wait(sem, count + 1)

    def load(self):
        loads = []
        for index, ref in enumerate(self.ins):
            copy = pltpu.make_async_copy(ref, self.stage[index], self.load_sem.at[index])
            copy.start()
            loads.append(copy)
        stores = []
        for index, copy in enumerate(loads):
            copy.wait()
            store = pltpu.make_async_copy(
                self.stage[index],
                self.outs[index].at[self.at["y"], self.at["x"], self.core, self.at["z"]],
                self.load_sem.at[index],
            )
            store.start()
            stores.append(store)
        for store in stores:
            store.wait()

    def region(self, index, done, axis, place, start, length):
        pick = {
            name: (pl.ds(0, self.sizes[name]) if name in done else self.at[name]) for name in "yxz"
        }
        if axis is not None:
            pick[axis] = place
        return self.outs[index].at[
            pick["y"], pick["x"], self.core, pick["z"], pl.ds(start, length)
        ]

    def copy(self, ref, where):
        slot = self.next_sem
        self.next_sem += 1
        return pltpu.make_async_remote_copy(
            src_ref=ref,
            dst_ref=ref,
            send_sem=self.send_sem.at[slot],
            recv_sem=self.recv_sem.at[slot],
            device_id=where,
            device_id_type=MESH_ID,
        )

    def steps(self, index, axes, start, length):
        steps = []
        pending = []
        for position, axis in enumerate(axes):
            size = self.sizes[axis]
            here = self.at[axis]
            done = axes[:position]
            for hop in range(1, size):
                sends, waits = [], []
                for move in (1, -1):
                    carried = here - move * (hop - 1)
                    can_send = (carried >= 0) & (carried < size)
                    can_send &= (here + move >= 0) & (here + move < size)
                    coming = here - move * hop
                    can_get = (coming >= 0) & (coming < size)
                    slot_ref = lambda place: self.region(index, done, axis, place, start, length)
                    safe = jnp.clip(carried, 0, size - 1)
                    other = jnp.clip(here + move, 0, size - 1) - here
                    copy = self.copy(slot_ref(safe), self.device(axis, other))
                    sends.append((can_send, copy))
                    waits.append((can_get, copy))
                steps.append((pending, sends))
                self.sends += sends
                pending = waits
        everything = self.region(index, axes, None, None, start, length)
        copy = self.copy(everything, self.device("core"))
        steps.append((pending, [(None, copy)]))
        self.sends.append((None, copy))
        steps.append(([(None, copy)], []))
        return steps

    def tick(self, time):
        for offset, steps in self.flows:
            step = time - offset
            if 0 <= step < len(steps):
                waits, sends = steps[step]
                for when, copy in waits:
                    run_if(when, copy.wait_recv)
                for when, copy in sends:
                    run_if(when, copy.start)

    def finish(self):
        for when, copy in self.sends:
            run_if(when, copy.wait_send)


def run_if(when, action):
    if when is None:
        action()
    else:
        pl.when(when)(lambda: action())


def count_copies(sizes, rows):
    hops = sum(2 * (sizes[axis] - 1) for axis in "yxz") + 1
    return sum(hops for count in rows for start, length in piece_rows(count, False) if length)


def gather_weights(mesh_shape, weights, order):
    outer, inner = split_lat(mesh_shape["lat"])
    sizes = {"y": outer, "x": inner, "z": mesh_shape["lon"]}
    total = len(weights)
    copies = count_copies(sizes, [weight.shape[0] for weight in weights])

    def kernel(*refs):
        ins, outs, scratch = refs[:total], refs[total : 2 * total], refs[2 * total :]
        stage = scratch[:total]
        send_sem, recv_sem, load_sem = scratch[total:]
        gather = Gather(sizes, ins, outs, stage, send_sem, recv_sem, load_sem, order)
        gather.load()
        gather.barrier()
        for time in range(gather.length):
            gather.tick(time)
        gather.finish()

    lead = (outer, inner, 2, mesh_shape["lon"])
    outs = pl.pallas_call(
        kernel,
        out_shape=[
            jax.ShapeDtypeStruct(lead + weight.shape, weight.dtype) for weight in weights
        ],
        in_specs=[pl.BlockSpec(memory_space=pl.ANY)] * total,
        out_specs=[pl.BlockSpec(memory_space=pl.ANY)] * total,
        scratch_shapes=[pltpu.VMEM(weight.shape, weight.dtype) for weight in weights]
        + [
            pltpu.SemaphoreType.DMA((copies,)),
            pltpu.SemaphoreType.DMA((copies,)),
            pltpu.SemaphoreType.DMA((total,)),
        ],
        compiler_params=pltpu.CompilerParams(collective_id=0, has_side_effects=True),
        cost_estimate=pl.CostEstimate(
            flops=90_000_000_000, bytes_accessed=50_000_000, transcendentals=0
        ),
    )(*weights)
    return [out.reshape(-1, out.shape[-1]) for out in outs]


def from_behind(value, axis, steps):
    count = lax.axis_size(axis)
    pairs = [(source, (source + steps) % count) for source in range(count)]
    return lax.ppermute(value, axis, pairs)


def layer_norm(values):
    widened = values.astype(jnp.float32)
    centre = jnp.mean(widened, axis=-1, keepdims=True)
    spread = jnp.mean(jnp.square(widened - centre), axis=-1, keepdims=True)
    return ((widened - centre) * lax.rsqrt(spread + 1e-05)).astype(jnp.bfloat16)


def offsets_table():
    cell_ids = jnp.arange(64, dtype=jnp.int32)
    row_of = cell_ids // 8
    col_of = cell_ids % 8
    return (row_of[:, None] - row_of[None, :] + 7) * 15 + (col_of[:, None] - col_of[None, :] + 7)


def row_region(row_ids, total_rows):
    return jnp.where(row_ids < 4, 2, jnp.where(row_ids >= total_rows - 4, 1, 0)).astype(jnp.int32)


def window_attention(queries, pair_cells, row_start, col_start, sea_mask, pos_bias):
    batch_size, row_count, col_count, feat_width = queries.shape
    head_count = pos_bias.shape[0]
    head_size = feat_width // head_count
    lat_cells, lon_cells = sea_mask.shape
    down_count = row_count // 8
    across_count = col_count // 8
    window_count = down_count * across_count

    def to_windows(values):
        last_dim = values.shape[-1]
        shaped = values.reshape(batch_size, down_count, 8, across_count, 8, last_dim)
        return shaped.transpose(0, 1, 3, 2, 4, 5).reshape(batch_size, window_count, 64, last_dim)

    query_win = to_windows(queries)
    pair_win = to_windows(pair_cells)
    grid_rows = (row_start + jnp.arange(row_count, dtype=jnp.int32)) % lat_cells
    region = row_region(grid_rows, lat_cells).reshape(down_count, 8)
    region = jnp.broadcast_to(region[:, None, :, None], (down_count, across_count, 8, 8)).reshape(
        window_count, 64
    )
    sea_tiled = jnp.tile(sea_mask, (2, 2))
    sea_keep = lax.dynamic_slice(
        sea_tiled, (row_start % lat_cells, col_start % lon_cells), (row_count, col_count)
    )
    sea_keep = (
        sea_keep.reshape(down_count, 8, across_count, 8)
        .transpose(0, 2, 1, 3)
        .reshape(window_count, 64)
        == 1
    )
    same_cell = jnp.eye(64, dtype=bool)
    allowed = (region[:, :, None] == region[:, None, :]) & (sea_keep[:, None, :] | same_cell[None])
    group_width = 4 * head_size
    score_scale = head_size ** (-0.5)

    def one_group(group_index):
        first_col = group_index * group_width
        split_shape = (batch_size, window_count, 64, 4, head_size)
        query_part = lax.dynamic_slice_in_dim(query_win, first_col, group_width, 3).reshape(
            split_shape
        )
        key_part = lax.dynamic_slice_in_dim(pair_win, first_col, group_width, 3).reshape(
            split_shape
        )
        value_part = lax.dynamic_slice_in_dim(
            pair_win, feat_width + first_col, group_width, 3
        ).reshape(split_shape)
        bias_part = lax.dynamic_slice_in_dim(pos_bias, group_index * 4, 4, 0)
        scores = jnp.einsum(
            "bsqhd,bskhd->bshqk", query_part, key_part, preferred_element_type=jnp.float32
        )
        scores = scores * score_scale + bias_part[None, None]
        scores = jnp.where(allowed[None, :, None], scores, -1e30)
        row_top = jnp.max(scores, axis=-1, keepdims=True)
        weights = jnp.exp(scores - row_top)
        attn_probs = (weights / jnp.sum(weights, axis=-1, keepdims=True)).astype(jnp.bfloat16)
        context = jnp.einsum(
            "bshqk,bskhd->bsqhd", attn_probs, value_part, preferred_element_type=jnp.float32
        )
        return context.astype(jnp.bfloat16).reshape(batch_size, window_count, 64, group_width)

    groups = lax.map(one_group, jnp.arange(head_count // 4, dtype=jnp.int32))
    context = jnp.transpose(groups, (1, 2, 3, 0, 4)).reshape(
        batch_size, down_count, across_count, 8, 8, feat_width
    )
    return context.transpose(0, 1, 3, 2, 4, 5).reshape(batch_size, row_count, col_count, feat_width)


def per_device(tokens, qkv_weight, proj_weight, up_weight, down_weight, bias_table, sea_mask):
    batch_size, lat_rows, lon_cols, feat_width = tokens.shape
    mesh_shape = {"lat": lax.axis_size("lat"), "lon": lax.axis_size("lon")}
    qkv_full, proj_full, up_full, down_full = gather_weights(
        mesh_shape,
        (qkv_weight, proj_weight, up_weight, down_weight),
        ((0, 0), (1, 1), (2, 2), (3, 4)),
    )
    head_count = bias_table.shape[1]
    row_base = lax.axis_index("lat") * lat_rows
    col_base = lax.axis_index("lon") * lon_cols
    offset_ids = offsets_table().reshape(-1)
    one_hot = (
        offset_ids[:, None] == jnp.arange(bias_table.shape[0], dtype=jnp.int32)[None, :]
    ).astype(jnp.float32)
    pos_bias = jnp.dot(one_hot, bias_table, precision=lax.Precision.HIGHEST)
    pos_bias = pos_bias.reshape(64, 64, head_count).transpose(2, 0, 1)
    normed = layer_norm(tokens)
    arrived = from_behind(normed[:, :4], "lat", -1)
    rolled_rows = jnp.concatenate([normed[:, 4:], arrived], axis=1)
    arrived_cols = from_behind(rolled_rows[:, :, :4], "lon", -1)
    feed_cells = jnp.concatenate([rolled_rows[:, :, 4:], arrived_cols], axis=2)
    feed_flat = feed_cells.reshape(-1, feat_width)
    projected = lax.dot_general(
        feed_flat,
        qkv_full,
        (((1,), (1,)), ((), ())),
        preferred_element_type=jnp.float32,
    ).astype(jnp.bfloat16)
    projected = projected.reshape(batch_size, lat_rows, lon_cols, 3 * feat_width)
    queries = projected[..., :feat_width]
    pair_cells = projected[..., feat_width:]
    rolled_context = window_attention(
        queries, pair_cells, row_base + 4, col_base + 4, sea_mask, pos_bias
    )
    came_cols = from_behind(rolled_context[:, :, lon_cols - 4 :], "lon", 1)
    back_cols = jnp.concatenate([came_cols, rolled_context[:, :, : lon_cols - 4]], axis=2)
    came_rows = from_behind(back_cols[:, lat_rows - 4 :], "lat", 1)
    context = jnp.concatenate([came_rows, back_cols[:, : lat_rows - 4]], axis=1)
    context_flat = context.reshape(-1, feat_width)
    attention_out = lax.dot_general(
        context_flat,
        proj_full,
        (((1,), (1,)), ((), ())),
        preferred_element_type=jnp.float32,
    )
    attended = (tokens.reshape(-1, feat_width).astype(jnp.float32) + attention_out).astype(
        jnp.bfloat16
    )
    normed_two = layer_norm(attended)
    hidden = lax.dot_general(
        normed_two, up_full, (((1,), (1,)), ((), ())), preferred_element_type=jnp.float32
    )
    hidden = jax.nn.gelu(hidden).astype(jnp.bfloat16)
    hidden_sum = jnp.dot(hidden, down_full, preferred_element_type=jnp.float32)
    result = (attended.astype(jnp.float32) + hidden_sum).astype(jnp.bfloat16)
    return result.reshape(tokens.shape)


def solution(mesh):
    placed = (
        P(None, "lat", "lon", None),
        P(("lat", "lon"), None),
        P(("lat", "lon"), None),
        P(("lat", "lon"), None),
        P(("lat", "lon"), None),
        P(),
        P(),
    )
    return jax.shard_map(
        per_device,
        mesh=mesh,
        in_specs=placed,
        out_specs=P(None, "lat", "lon", None),
        check_vma=False,
    )
```
